32 devices in a mesh: variant: 4 (over x, core), mesh: 8 (over z, y).
Axes of the slice: x: 2, y: 2, z: 4, core: 2. Of those that a mesh axis runs over, the one named last changes fastest.
Arguments:
- snapshots: float32 [4, 64, 131072], P('variant', None, 'mesh'), may hold values from -12 to 12, as said below
- ref_index: int32 [1], replicated, may hold values from 0 to 3
- weight_codes: int32 [4], replicated, may hold values from 1 to 16
Outputs:
- new_basis: float32 [64, 131072], P(None, 'mesh')
The draws below stay inside these ranges and needn't reach their ends.
Inputs may be any that keep to these rules, and one draw needn't show every extreme that they name: `snapshots`: each variant's snapshot matrix has full rank 64, and the principal angles between any two variants' spans have tangents below 0.8.
All inputs are finite; a program needn't handle non-finite values.
Results may differ from the reference program's by a relative error of at most 0.0001.
Values sent between devices are 32-bit elements; how exact they have to be, the bound alone decides.
No kernel may reach another device: no remote copies, remote signals or barrier semaphores. Data moves between devices by JAX's collectives and lax.ppermute only.
A program may use at most 64 MiB of HBM per device.

```python
import math
import jax
import jax.numpy as jnp
from jax import lax

K = 64
NROWS = 131072
V = 4


def draw_snapshots(key, part):
    first = jax.random.fold_in(jax.random.fold_in(key, 11), 0)
    second = jax.random.fold_in(jax.random.fold_in(key, 11), 1)
    fourth = jax.random.fold_in(jax.random.fold_in(key, 11), 3)
    amplitude = 0.45 * jnp.exp(jax.random.uniform(fourth, (V, K, 1), jnp.float32, jnp.log(0.02 / 0.45), 0.0))
    position = jnp.arange(NROWS, dtype=jnp.float32) / jnp.float32(max(NROWS - 1, 1))
    rising = jnp.exp(jnp.log(4.0) * position)
    base = jax.random.normal(first, (K, NROWS), jnp.float32)
    noise = jax.random.normal(second, (V, K, NROWS), jnp.float32)
    rising = rising / jnp.sqrt(jnp.mean(rising * rising))
    noise = noise * rising[None, None, :]
    return jnp.clip(base[None] + amplitude * noise, -12.0, 12.0)


def place_ends(array, stream_key, smallest, largest):
    extent = array.shape
    index_at = [jax.random.randint(jax.random.fold_in(stream_key, axis), (), 0, extent[axis]) for axis in range(len(extent))]
    array = array.at[tuple(index_at)].set(smallest)
    longest = extent.index(max(extent))
    index_at[longest] = (index_at[longest] + 1) % extent[longest]
    return array.at[tuple(index_at)].set(largest)


def setup_inputs(seed: int = 0) -> dict:
    key_of = jax.random.split(jax.random.key(seed), 4)
    snapshots = draw_snapshots(jax.random.fold_in(key_of[3], 71), 0)
    ref_index = jax.random.randint(key_of[1], (1,), 0, V).astype(jnp.int32)
    weight_codes = place_ends(jax.random.randint(key_of[2], (V,), 1, 17), jax.random.fold_in(key_of[2], 1), 1, 16).astype(jnp.int32)
    return dict(snapshots=snapshots, ref_index=ref_index, weight_codes=weight_codes)


highest = lax.Precision.HIGHEST
atan_coeffs = [(-1.0) ** k / (2 * k + 1) for k in range(24)]
cos_coeffs = [(-1.0) ** k / math.factorial(2 * k) for k in range(24)]
sin_coeffs = [(-1.0) ** k / math.factorial(2 * k + 1) for k in range(24)]

def product(left, right):
    return jnp.dot(left.astype(jnp.float32), right.astype(jnp.float32), precision=highest, preferred_element_type=jnp.float32)

def series(matrix, coeffs):
    eye = jnp.eye(matrix.shape[0], dtype=jnp.float32)
    total = coeffs[-1] * eye
    for coeff in reversed(coeffs[:-1]):
        total = coeff * eye + product(matrix, total)
    return total

def orthonormal(snap):
    lower = jnp.linalg.cholesky(product(snap, snap.T))
    return jax.scipy.linalg.solve_triangular(lower, snap, lower=True)

def reference(snapshots, ref_index, weight_codes):
    base_ref = orthonormal(lax.dynamic_index_in_dim(snapshots, ref_index[0].astype(jnp.int32), 0, keepdims=False))
    codes = weight_codes.astype(jnp.float32)
    weights = codes / jnp.sum(codes)
    blended = jnp.zeros(base_ref.shape, jnp.float32)
    for variant in range(V):
        base_own = orthonormal(snapshots[variant])
        minv = jnp.linalg.inv(product(base_ref, base_own.T))
        tangent = product(minv.T, base_own) - base_ref
        factor = series(product(tangent, tangent.T), atan_coeffs)
        blended = blended + weights[variant] * product(factor, tangent)
    energy = product(blended, blended.T)
    mixed = product(series(energy, cos_coeffs), base_ref) + product(series(energy, sin_coeffs), blended)
    return mixed * jnp.float32(math.sqrt(NROWS))
```

```python
import functools
import math

import jax
import jax.numpy as jnp
from jax import lax
from jax.experimental import pallas as pl
from jax.experimental.pallas import tpu as pltpu
from jax.sharding import PartitionSpec as P


highest = lax.Precision.HIGHEST
atan_coeffs = [(-1.0) ** k / (2 * k + 1) for k in range(24)]
cos_coeffs = [(-1.0) ** k / math.factorial(2 * k) for k in range(24)]
sin_coeffs = [(-1.0) ** k / math.factorial(2 * k + 1) for k in range(24)]

CORES = 2
LOWEST = 1.0 / 1.64
STEP = 6


def xor_pairs(size, offset):
    return [(i, i ^ offset) for i in range(size)]


def mm(a, b):
    return jnp.dot(a, b, precision=highest, preferred_element_type=jnp.float32)


def mmt(a, b):
    return lax.dot_general(
        a, b, (((1,), (1,)), ((), ())), precision=highest, preferred_element_type=jnp.float32
    )


def powers_of(matrix, top):
    powers = {1: matrix}
    for k in range(2, top + 1):
        powers[k] = mm(powers[k // 2], powers[k - k // 2])
    return powers


def split(x):
    high = x.astype(jnp.bfloat16)
    rest = x - high.astype(jnp.float32)
    middle = rest.astype(jnp.bfloat16)
    low = (rest - middle.astype(jnp.float32)).astype(jnp.bfloat16)
    return high, middle, low


def raw_gram(a, b):
    return lax.dot_general(a, b, (((1,), (1,)), ((), ())), preferred_element_type=jnp.float32)


def fold(total, rows):
    tall = total.shape[0] // 3
    part = lambda i, j: total[i * tall:(i + 1) * tall, j * rows:(j + 1) * rows]
    order = sorted(((i, j) for i in range(3) for j in range(3)), key=lambda ij: -sum(ij))
    result = part(*order[0])
    for ij in order[1:]:
        result = result + part(*ij)
    return result


def gram_kernel(heads, groups, prior, where, *refs):
    count = heads + max(groups) + (1 if prior else 0)
    refs_in, out, totals = refs[:count], refs[count], refs[count + 1:]
    step, last = pl.program_id(0), pl.num_programs(0) - 1
    cols = refs_in[heads:heads + max(groups)]
    size = cols[0].shape[0]
    pieces = [split(col[...]) for col in cols]

    @pl.when(step == 0)
    def _():
        for total in totals:
            total[...] = jnp.zeros_like(total)

    for head in range(heads):
        right = jnp.concatenate(split(refs_in[head][...]), axis=0)
        left = jnp.concatenate(
            [pieces[g][level] for level in range(3) for g in range(groups[head])], axis=0
        )
        totals[head][...] += raw_gram(left, right)

    @pl.when(step == last)
    def _():
        blocks = []
        for head in range(heads):
            result = fold(totals[head][...], size)
            blocks += [result[g * size:(g + 1) * size] for g in range(groups[head])]
        result = jnp.concatenate(blocks, axis=1)
        out[...] = result + refs_in[count - 1][...] if prior else result


def gram(place, heads, whole, cols, groups, before, extent, tile):
    size = whole[0].shape[0]
    tile = min(tile, extent)
    steps = extent // tile
    width = sum(groups) * size
    at_place = pl.BlockSpec((size, tile), lambda i, w: (0, w[0] * steps + i))
    at_start = pl.BlockSpec((size, tile), lambda i, w: (0, i))
    block = pl.BlockSpec((size, width), lambda i, w: (0, 0))
    operands = [*heads, *whole, *cols]
    specs = [at_start] * len(heads) + [at_place] * len(whole) + [at_start] * len(cols)
    if before is not None:
        operands.append(before)
        specs.append(block)
    return pl.pallas_call(
        functools.partial(gram_kernel, len(heads), groups, before is not None),
        out_shape=jax.ShapeDtypeStruct((size, width), jnp.float32),
        grid_spec=pltpu.PrefetchScalarGridSpec(
            num_scalar_prefetch=1,
            grid=(steps,),
            in_specs=specs,
            out_specs=block,
            scratch_shapes=[pltpu.VMEM((3 * g * size, 3 * size), jnp.float32) for g in groups],
        ),
        cost_estimate=pl.CostEstimate(
            flops=9 * 2 * size * width * extent, transcendentals=0,
            bytes_accessed=4 * (len(operands)) * size * extent,
        ),
    )(place, *operands)


def diagonal(packed, mask):
    return jnp.where(mask, jnp.concatenate([packed] * (mask.shape[0] // packed.shape[0]), axis=0), 0.0)


def small_kernel(n, scale, root_ref, weight_ref, *refs):
    gathered = refs[:n]
    out, corr = refs[n], refs[n + 1]
    size = out.shape[0]
    root = root_ref[0]
    rows = lax.broadcasted_iota(jnp.int32, (size, size), 0)
    cols = lax.broadcasted_iota(jnp.int32, (size, size), 1)
    eye = (rows == cols).astype(jnp.float32)
    inv_lower = [gathered[j][:size, :size] for j in range(n)]
    known = {}

    def add(row, col, block):
        if row > col:
            row, col, block = col, row, block.T
        known[row, col] = block if (row, col) not in known else known[row, col] + block

    for s in range(0, n, CORES):
        for g in range(1, CORES):
            add(s ^ g, s, gathered[s][:size, g * size:(g + 1) * size])
    for s in range(n):
        chip, core = s // CORES, s % CORES
        column = 0
        for head in range(1, n // CORES):
            for other in range(head):
                for g in range(CORES):
                    block = gathered[s][size:, column * size:(column + 1) * size]
                    add(CORES * (other ^ chip) + (core ^ g), CORES * (head ^ chip) + core, block)
                    column += 1
    for j in range(n):
        corr[j, j] = eye
        for i in range(j + 1, n):
            block = mmt(mm(inv_lower[j], known[j, i]), inv_lower[i])
            corr[j, i] = block
            corr[i, j] = block.T
    middle = 2.0 / (1.0 + LOWEST)
    group = min(n, 4)
    wide = group * size
    mask = (
        lax.broadcasted_iota(jnp.int32, (wide, wide), 0) // size
        == lax.broadcasted_iota(jnp.int32, (wide, wide), 1) // size
    )
    eyes = jnp.concatenate([eye] * group, axis=1)
    lane = lax.broadcasted_iota(jnp.int32, (size, wide), 1) // size
    terms, phi = [], jnp.zeros((size, size), jnp.float32)

    def each(a, b):
        return mm(a, diagonal(b, mask))

    for first in range(0, n, group):
        m = [corr[root, first + g] for g in range(group)]
        k = jnp.concatenate([mmt(block, block) for block in m], axis=1)
        m = jnp.concatenate(m, axis=1)
        r = eyes - middle * k
        r2 = each(r, r)
        total = each(eyes + r, eyes + r2)
        r4 = each(r2, r2)
        total = each(total, eyes + r4)
        r8 = each(r4, r4)
        inv = middle * each(total, eyes + r8)
        inv = inv + each(inv, eyes - each(k, inv))
        right = each(inv, m)
        powers = {1: inv - eyes}
        for p in range(2, STEP + 1):
            powers[p] = each(powers[p // 2], powers[p - p // 2])
        factor = None
        for start in reversed(range(0, len(atan_coeffs), STEP)):
            block = atan_coeffs[start] * eyes
            for p in range(1, min(STEP, len(atan_coeffs) - start)):
                block = block + atan_coeffs[start + p] * powers[p]
            factor = block if factor is None else block + each(powers[STEP], factor)
        weight = jnp.zeros((size, wide), jnp.float32)
        for g in range(group):
            weight = jnp.where(lane == g, weight_ref[first + g], weight)
        factor = weight * factor
        term = each(factor, right)
        for g in range(group):
            phi = phi + factor[:, g * size:(g + 1) * size]
            terms.append(term[:, g * size:(g + 1) * size])
    energy = -mm(phi, phi)
    for j in range(n):
        column = terms[j].T
        for i in range(n):
            if i != j:
                column = column + mmt(corr[j, i], terms[i])
        energy = energy + mm(terms[j], column)
    right = []
    for j in range(n):
        right.append(mm(terms[j] - jnp.where(root == j, 1.0, 0.0) * phi, inv_lower[j]))
    lead = [jnp.where(root == j, 1.0, 0.0) * inv_lower[j] for j in range(n)]
    powers = powers_of(energy, STEP)
    both = [
        jnp.concatenate([jnp.full((1, size), c), jnp.full((1, size), s)], axis=1)
        for c, s in zip(cos_coeffs, sin_coeffs)
    ]
    twice = {p: jnp.concatenate([power] * 2, axis=1) for p, power in powers.items()}
    total = None
    for start in reversed(range(0, len(both), STEP)):
        block = both[start] * jnp.concatenate([eye] * 2, axis=1)
        for p in range(1, min(STEP, len(both) - start)):
            block = block + both[start + p] * twice[p]
        total = block if total is None else block + mm(powers[STEP], total)
    stacked = jnp.concatenate(
        [jnp.concatenate(lead, axis=1), jnp.concatenate(right, axis=1)], axis=0
    )
    out[...] = scale * mm(total, stacked)


def small(root, weights, gathered, size, scale):
    n = len(gathered)
    vmem = pl.BlockSpec(memory_space=pltpu.VMEM)
    smem = pl.BlockSpec(memory_space=pltpu.SMEM)
    return pl.pallas_call(
        functools.partial(small_kernel, n, scale),
        out_shape=jax.ShapeDtypeStruct((size, n * size), jnp.float32),
        in_specs=[smem, smem] + [vmem] * n,
        out_specs=vmem,
        scratch_shapes=[pltpu.VMEM((n, n, size, size), jnp.float32)],
        cost_estimate=pl.CostEstimate(
            flops=20000 * size**3, bytes_accessed=4 * 4 * n * size * size, transcendentals=0
        ),
        name="small",
    )(root, weights, *gathered)


def mix_kernel(n, where, coeffs, *refs):
    pieces, out = refs[:n], refs[-1]
    size = out.shape[0]
    high, middle, low = split(jnp.concatenate([piece[...] for piece in pieces], axis=0))
    left = jnp.concatenate(split(coeffs[...]), axis=0)
    first = jnp.dot(left, high, preferred_element_type=jnp.float32)
    second = jnp.dot(left[:2 * size], middle, preferred_element_type=jnp.float32)
    third = jnp.dot(left[:size], low, preferred_element_type=jnp.float32)
    small_part = first[2 * size:] + second[size:] + third
    out[...] = (small_part + (first[size:2 * size] + second[:size])) + first[:size]


def mix(place, coeffs, whole, parts, result, tile):
    size, cols = whole[0].shape
    part = parts[0].shape[1]
    tile = min(tile, part)
    steps = part // tile
    n = len(whole) + len(parts)
    at_place = pl.BlockSpec((size, tile), lambda i, w: (0, w[0] * steps + i))
    at_start = pl.BlockSpec((size, tile), lambda i, w: (0, i))
    specs = [pl.BlockSpec((size, n * size), lambda i, w: (0, 0))]
    specs += [at_place] * len(whole) + [at_start] * len(parts)
    operands = [place, coeffs, *whole, *parts]
    aliases = {}
    if result is not None:
        specs.append(pl.BlockSpec(memory_space=pl.ANY))
        aliases = {len(operands): 0}
        operands.append(result)
    return pl.pallas_call(
        functools.partial(mix_kernel, n),
        out_shape=jax.ShapeDtypeStruct((size, cols), jnp.float32),
        grid_spec=pltpu.PrefetchScalarGridSpec(
            num_scalar_prefetch=1, grid=(steps,), in_specs=specs, out_specs=at_place
        ),
        input_output_aliases=aliases,
        cost_estimate=pl.CostEstimate(
            flops=6 * 2 * n * size * size * part, bytes_accessed=4 * (n + 1) * size * part,
            transcendentals=0,
        ),
        name="mix",
    )(*operands)


def after(x, *deps):
    return lax.optimization_barrier((x, *deps))[0]


def counts(chips):
    return max(1, 4 // chips), max(1, 8 // chips)


def early_of(chips, far_count):
    return (chips - 1) ** 2 * far_count // 2


def on_device(snapshots, ref_index, weight_codes):
    own = snapshots[0]
    size, cols = own.shape
    n, mesh_size = lax.axis_size("variant"), lax.axis_size("mesh")
    chips = n // CORES
    part = cols // chips
    me = lax.axis_index("variant").astype(jnp.int32)
    chip = me // CORES
    near_count, far_count = counts(chips)
    early = early_of(chips, far_count)
    scale = math.sqrt(cols * mesh_size)
    codes = weight_codes.astype(jnp.float32)
    weights = (codes / jnp.sum(codes))[jnp.arange(n) ^ me]
    root = ref_index ^ me

    def move(x, offset):
        return lax.ppermute(x, "variant", xor_pairs(n, offset))

    def mesh_sum(x):
        step = 1
        while step < mesh_size:
            x = x + lax.ppermute(x, "mesh", xor_pairs(mesh_size, step))
            step *= 2
        return x

    def gather(x):
        both = jnp.concatenate([x, move(x, 1)], axis=0)
        blocks = [both]
        for offset in range(1, chips):
            blocks.append(move(both, CORES * offset))
        rows = x.shape[0]
        return [b[g * rows:(g + 1) * rows] for b in blocks for g in range(CORES)]

    def pieces_of(x, count, index, offset):
        chunk = part // count
        return lax.dynamic_slice(x, (0, (chip ^ offset) * part + index * chunk), (size, chunk))

    near, far = {}, {}
    source = own
    for c in range(near_count):
        for o in range(1, chips):
            piece = pieces_of(source, near_count, c, o)
            source = after(own, piece)
            near[o, c] = move(piece, CORES * o)
    partner = move(own, 1)
    for p in range(1, chips):
        for c in range(far_count):
            for o in range(1, chips):
                piece = pieces_of(source, far_count, c, o ^ p)
                far[o, p, c] = move(piece, CORES * o)
    zero = jnp.zeros((1,), jnp.int32)
    own_gram = gram(zero, [own], [own, partner], [], [CORES], None, cols, 4096)
    own_gram = mesh_sum(own_gram)
    lower = jnp.linalg.cholesky(own_gram[:, :size])
    inv_lower = jax.scipy.linalg.solve_triangular(lower, jnp.eye(size, dtype=jnp.float32), lower=True)
    ready = jnp.concatenate([inv_lower, own_gram[:, size:]], axis=1)

    cross = None
    others = {}
    for c in range(near_count):
        heads = [after(near[o, c], ready) for o in range(1, chips)]
        for o in range(1, chips):
            near[o, c] = heads[o - 1]
        columns = []
        for o in range(1, chips - 1):
            others[o, c] = move(near[o, c], 1)
            columns += [near[o, c], others[o, c]]
        cross = gram(
            (chip * near_count + c)[None], heads, [own, partner], columns,
            [CORES * o for o in range(1, chips)], cross, part // near_count, 2048,
        )
    cross = mesh_sum(cross)
    width = max(cross.shape[1], ready.shape[1])
    wide = lambda x: jnp.pad(x, ((0, 0), (0, width - x.shape[1])))
    gathered = gather(jnp.concatenate([wide(ready), wide(cross)], axis=0))
    coeffs = small(root, weights, gathered, size, scale)

    def forward(x, *deps):
        return move(after(x, *deps), 1)

    result = None
    for c in range(near_count):
        parts = []
        for o in range(1, chips):
            other = others[o, c] if (o, c) in others else forward(near[o, c], gathered[-1])
            parts += [near[o, c], other]
        result = mix((chip * near_count + c)[None], coeffs, [own, partner], parts, result, 2048)
    for p in range(1, chips):
        for c in range(far_count):
            parts = []
            for o in range(1, chips):
                number = (p - 1) * far_count * (chips - 1) + c * (chips - 1) + o - 1
                dep = gathered[-1] if number < early else coeffs
                parts += [far[o, p, c], forward(far[o, p, c], dep)]
            result = mix(((chip ^ p) * far_count + c)[None], coeffs, [own, partner], parts, result, 2048)
    return result


def solution(mesh):
    return jax.shard_map(
        on_device,
        mesh=mesh,
        in_specs=(P("variant", None, "mesh"), P(), P()),
        out_specs=P(None, "mesh"),
        check_vma=False,
    )
```

```python
import functools
import math

import jax
import jax.numpy as jnp
from jax import lax
from jax.experimental import pallas as pl
from jax.experimental.pallas import tpu as pltpu
from jax.sharding import PartitionSpec as P


highest = lax.Precision.HIGHEST
atan_coeffs = [(-1.0) ** k / (2 * k + 1) for k in range(24)]
cos_coeffs = [(-1.0) ** k / math.factorial(2 * k) for k in range(24)]
sin_coeffs = [(-1.0) ** k / math.factorial(2 * k + 1) for k in range(24)]

CORES = 2
LOWEST = 1.0 / 1.64
STEP = 6


def xor_pairs(size, offset):
    return [(i, i ^ offset) for i in range(size)]


def mm(a, b):
    return jnp.dot(a, b, precision=highest, preferred_element_type=jnp.float32)


def mmt(a, b):
    return lax.dot_general(
        a, b, (((1,), (1,)), ((), ())), precision=highest, preferred_element_type=jnp.float32
    )


def powers_of(matrix, top):
    powers = {1: matrix}
    for k in range(2, top + 1):
        powers[k] = mm(powers[k // 2], powers[k - k // 2])
    return powers


def split(x):
    high = x.astype(jnp.bfloat16)
    rest = x - high.astype(jnp.float32)
    middle = rest.astype(jnp.bfloat16)
    low = (rest - middle.astype(jnp.float32)).astype(jnp.bfloat16)
    return high, middle, low


def raw_gram(a, b):
    return lax.dot_general(a, b, (((1,), (1,)), ((), ())), preferred_element_type=jnp.float32)


def raw_product(a, b):
    return jnp.dot(a, b, preferred_element_type=jnp.float32)


def fold(total, rows):
    tall = total.shape[0] // 3
    part = lambda i, j: total[i * tall:(i + 1) * tall, j * rows:(j + 1) * rows]
    order = sorted(((i, j) for i in range(3) for j in range(3)), key=lambda ij: -sum(ij))
    result = part(*order[0])
    for ij in order[1:]:
        result = result + part(*ij)
    return result


def load(refs, starts, slots, sems, tile):
    steps = slots[0].shape[1] // tile
    waits = []
    for t in range(steps):
        copies = []
        for index, (ref, start, slot) in enumerate(zip(refs, starts, slots)):
            first = start + t * tile
            if not isinstance(first, int):
                first = pl.multiple_of(first, 128)
            copies.append(
                pltpu.make_async_copy(
                    ref.at[:, pl.ds(first, tile)], slot.at[:, pl.ds(t * tile, tile)], sems.at[index, t]
                )
            )
            copies[-1].start()
        waits.append(copies)
    return waits


def gram_kernel(heads, groups, prior, at, whole, tile, where, *refs):
    count = (len(refs) - 2 - (1 if prior else 0)) // 2
    loaded, out = refs[:count], refs[count + (1 if prior else 0)]
    slots, sems = refs[-1 - count:-1], refs[-1]
    size, extent = slots[0].shape
    start = at(where) * extent
    waits = load(loaded, [start] * whole + [0] * (count - whole), slots, sems, tile)
    totals = [None] * len(heads)
    for t, copies in enumerate(waits):
        for copy in copies:
            copy.wait()
        pieces = [split(slot[:, t * tile:(t + 1) * tile]) for slot in slots]
        for index, (head, columns) in enumerate(zip(heads, groups)):
            right = jnp.concatenate(pieces[head], axis=0)
            left = jnp.concatenate([pieces[g][level] for level in range(3) for g in columns], axis=0)
            value = raw_gram(left, right)
            totals[index] = value if totals[index] is None else totals[index] + value
    blocks = []
    for columns, total in zip(groups, totals):
        result = fold(total, size)
        blocks += [result[g * size:(g + 1) * size] for g in range(len(columns))]
    result = jnp.concatenate(blocks, axis=1)
    out[...] = result + refs[count][...] if prior else result


def gram(where, at, whole, parts, heads, groups, before, extent, tile):
    size = (whole + parts)[0].shape[0]
    tile = min(tile, extent)
    width = sum(len(columns) for columns in groups) * size
    operands = [*whole, *parts]
    count = len(operands)
    vmem = pl.BlockSpec(memory_space=pltpu.VMEM)
    specs = [pl.BlockSpec(memory_space=pltpu.SMEM)] + [pl.BlockSpec(memory_space=pl.ANY)] * count
    if before is not None:
        operands.append(before)
        specs.append(vmem)
    return pl.pallas_call(
        functools.partial(gram_kernel, heads, groups, before is not None, at, len(whole), tile),
        out_shape=jax.ShapeDtypeStruct((size, width), jnp.float32),
        in_specs=specs,
        out_specs=vmem,
        scratch_shapes=[pltpu.VMEM((size, extent), jnp.float32)] * count
        + [pltpu.SemaphoreType.DMA((count, extent // tile))],
        cost_estimate=pl.CostEstimate(
            flops=9 * 2 * size * width * extent, transcendentals=0,
            bytes_accessed=4 * count * size * extent,
        ),
    )(where, *operands)


def invert_kernel(ref, out):
    size = ref.shape[0]
    rows = lax.broadcasted_iota(jnp.int32, (size, size), 0)
    cols = lax.broadcasted_iota(jnp.int32, (size, size), 1)
    eye = (rows == cols).astype(jnp.float32)
    index = lax.broadcasted_iota(jnp.int32, (size, 1), 0)
    work = jnp.concatenate([ref[:, :size], eye], axis=1)
    for j in range(size - 1):
        row = work[j:j + 1, :]
        factor = jnp.where(index > j, work[:, j:j + 1] / row[:, j:j + 1], 0.0)
        work = work - factor * row
    pivots = jnp.sum(work[:, :size] * eye, axis=1, keepdims=True)
    out[:, :size] = work[:, size:] / jnp.sqrt(pivots)
    out[:, size:] = ref[:, size:]


def invert(matrix):
    vmem = pl.BlockSpec(memory_space=pltpu.VMEM)
    return pl.pallas_call(
        invert_kernel,
        out_shape=jax.ShapeDtypeStruct(matrix.shape, jnp.float32),
        in_specs=[vmem],
        out_specs=vmem,
        cost_estimate=pl.CostEstimate(
            flops=4000 * matrix.shape[0] ** 2, bytes_accessed=8 * matrix.size, transcendentals=0
        ),
        name="invert",
    )(matrix)


def diagonal(packed, mask):
    return jnp.where(mask, jnp.concatenate([packed] * (mask.shape[0] // packed.shape[0]), axis=0), jnp.zeros((), packed.dtype))


def small_kernel(n, scale, me_ref, root_ref, code_ref, *refs):
    chips = n // CORES
    gathered, (out, gram_ref, corr) = refs[:chips], refs[chips:]
    size = out.shape[0]
    rows = gathered[0].shape[0] // CORES
    me = me_ref[0]
    root = root_ref[0] ^ me
    codes = [code_ref[j ^ me] for j in range(n)]
    eye = (
        lax.broadcasted_iota(jnp.int32, (size, size), 0)
        == lax.broadcasted_iota(jnp.int32, (size, size), 1)
    ).astype(jnp.float32)
    known = {}

    def add(row, col, block):
        if row > col:
            row, col, block = col, row, block.T
        known[row, col] = block if (row, col) not in known else known[row, col] + block

    lowers = []
    for s in range(n):
        chip, core = s // CORES, s % CORES
        ref, top = gathered[chip], core * rows
        lowers.append(ref[top:top + size, :size])
        add(s ^ 1, s, ref[top:top + size, size:CORES * size])
        column = 0
        for head in range(1, chips):
            for other in range(head):
                for g in range(CORES):
                    block = ref[top + size:top + 2 * size, column * size:(column + 1) * size]
                    add(CORES * (other ^ chip) + (core ^ g), CORES * (head ^ chip) + core, block)
                    column += 1
    zero = jnp.zeros((size, size), jnp.float32)
    for j in range(n):
        line = [zero if i == j else known[j, i] if j < i else known[i, j].T for i in range(n)]
        gram_ref[j * size:(j + 1) * size, :] = jnp.concatenate(line, axis=1)

    def block_mask(count):
        shape = (count * size, count * size)
        return (
            lax.broadcasted_iota(jnp.int32, shape, 0) // size
            == lax.broadcasted_iota(jnp.int32, shape, 1) // size
        )

    group = CORES
    wide = group * size
    every, mask = block_mask(n), block_mask(group)
    lower = jnp.concatenate(lowers, axis=1)
    spread = diagonal(lower, every)
    shape = (n * size, n * size)
    whole_eye = (
        lax.broadcasted_iota(jnp.int32, shape, 0) == lax.broadcasted_iota(jnp.int32, shape, 1)
    ).astype(jnp.float32)
    corr[...] = jnp.where(every, whole_eye, mmt(mm(spread, gram_ref[...]), spread))
    to_root = corr[pl.ds(pl.multiple_of(root * size, size), size), :]

    middle = 2.0 / (1.0 + LOWEST)
    eyes = jnp.concatenate([eye] * group, axis=1)
    lane = lax.broadcasted_iota(jnp.int32, (1, wide), 1) // size

    def each(a, b, product=raw_product):
        high, middle, low = [diagonal(x, mask) for x in split(b)]
        left = jnp.concatenate(split(a), axis=0)
        one = product(left, jnp.concatenate([high, middle], axis=product is raw_product))
        two = product(left[:size], low)
        little = one[2 * size:, :wide] + one[size:2 * size, wide:] + two
        return (little + (one[size:2 * size, :wide] + one[:size, wide:])) + one[:size, :wide]

    def groups(x):
        return [x[:, first * size:first * size + wide] for first in range(0, n, group)]

    terms, phi = [], zero
    for number, m in enumerate(groups(to_root)):
        k = each(m, m, raw_gram)
        r = eyes - middle * k
        r2 = each(r, r)
        total = each(eyes + r, eyes + r2)
        r4 = each(r2, r2)
        total = each(total, eyes + r4)
        r8 = each(r4, r4)
        inv = middle * each(total, eyes + r8)
        right = each(inv, m)
        powers = {1: inv - eyes}
        for p in range(2, STEP + 1):
            powers[p] = each(powers[p // 2], powers[p - p // 2])
        factor = None
        for start in reversed(range(0, len(atan_coeffs), STEP)):
            block = atan_coeffs[start] * eyes
            for p in range(1, min(STEP, len(atan_coeffs) - start)):
                block = block + atan_coeffs[start + p] * powers[p]
            factor = block if factor is None else block + each(powers[STEP], factor)
        weight = jnp.zeros((1, wide), jnp.int32)
        for g in range(group):
            weight = jnp.where(lane == g, codes[number * group + g], weight)
        all_codes = jnp.full((1, wide), sum(codes), jnp.int32)
        factor = (weight.astype(jnp.float32) / all_codes.astype(jnp.float32)) * factor
        for g in range(group):
            phi = phi + factor[:, g * size:(g + 1) * size]
        terms.append(each(factor, right))
    term = jnp.concatenate(terms, axis=1)
    energy = mmt(mm(term, corr[...]), term) - mm(phi, phi)
    at_root = lax.broadcasted_iota(jnp.int32, (1, n * size), 1) // size == root
    term = term - jnp.where(at_root, jnp.concatenate([phi] * n, axis=1), 0.0)
    right = [each(a, b) for a, b in zip(groups(term), groups(lower))]
    stacked = jnp.concatenate(
        [jnp.where(at_root, lower, 0.0), jnp.concatenate(right, axis=1)], axis=0
    )
    powers = powers_of(energy, STEP)
    both = [
        jnp.concatenate([jnp.full((1, size), c), jnp.full((1, size), s)], axis=1)
        for c, s in zip(cos_coeffs, sin_coeffs)
    ]
    twice = {p: jnp.concatenate([power] * 2, axis=1) for p, power in powers.items()}
    total = None
    for start in reversed(range(0, len(both), STEP)):
        block = both[start] * jnp.concatenate([eye] * 2, axis=1)
        for p in range(1, min(STEP, len(both) - start)):
            block = block + both[start + p] * twice[p]
        total = block if total is None else block + mm(powers[STEP], total)
    out[...] = scale * mm(total, stacked)


def small(me, root, codes, gathered, size, scale):
    n = len(gathered) * CORES
    vmem = pl.BlockSpec(memory_space=pltpu.VMEM)
    smem = pl.BlockSpec(memory_space=pltpu.SMEM)
    return pl.pallas_call(
        functools.partial(small_kernel, n, scale),
        out_shape=jax.ShapeDtypeStruct((size, n * size), jnp.float32),
        in_specs=[smem, smem, smem] + [vmem] * len(gathered),
        out_specs=vmem,
        scratch_shapes=[pltpu.VMEM((n * size, n * size), jnp.float32)] * 2,
        cost_estimate=pl.CostEstimate(
            flops=20000 * size**3, bytes_accessed=4 * 4 * n * size * size, transcendentals=0
        ),
        name="small",
    )(me, root, codes, *gathered)


def mix_kernel(whole, chunks, tile, aliased, where, coeffs, *refs):
    loaded = refs[:whole + sum(count for _, count, _ in chunks)]
    slots = refs[-3 - whole - chunks[0][1]:-3]
    out, (sums, in_sems, out_sems) = refs[len(loaded) + aliased], refs[-3:]
    size = sums.shape[0]
    waits, places, begun = [], [], whole
    for at, count, width in chunks:
        group = loaded[:whole] + loaded[begun:begun + count]
        begun += count
        for t in range(width // tile):
            number, copies = len(waits), []
            place = pl.ds(pl.multiple_of(at(where) + t * tile, 128), tile)
            for index, (ref, slot) in enumerate(zip(group, slots)):
                copies.append(
                    pltpu.make_async_copy(
                        ref.at[:, place if index < whole else pl.ds(t * tile, tile)],
                        slot.at[:, pl.ds(number * tile, tile)],
                        in_sems.at[index, number],
                    )
                )
                copies[-1].start()
            waits.append(copies)
            places.append(place)
    left = jnp.concatenate(split(coeffs[...]), axis=0)
    stores = []
    for t, copies in enumerate(waits):
        for copy in copies:
            copy.wait()
        here = slice(t * tile, (t + 1) * tile)
        high, middle, low = split(jnp.concatenate([slot[:, here] for slot in slots], axis=0))
        one = jnp.dot(left, high, preferred_element_type=jnp.float32)
        two = jnp.dot(left[:2 * size], middle, preferred_element_type=jnp.float32)
        three = jnp.dot(left[:size], low, preferred_element_type=jnp.float32)
        little = one[2 * size:] + two[size:] + three
        sums[:, here] = (little + (one[size:2 * size] + two[:size])) + one[:size]
        stores.append(
            pltpu.make_async_copy(
                sums.at[:, pl.ds(t * tile, tile)],
                out.at[:, places[t]],
                out_sems.at[t],
            )
        )
        stores[-1].start()
    for store in stores:
        store.wait()


def mix(where, coeffs, whole, chunks, result, tile):
    size, cols = whole[0].shape
    n = len(whole) + len(chunks[0][1])
    layout, extent, operands = [], 0, []
    for at, parts in chunks:
        layout.append((at, len(parts), parts[0].shape[1]))
        extent += parts[0].shape[1]
        operands += parts
    hbm = pl.BlockSpec(memory_space=pl.ANY)
    vmem = pl.BlockSpec(memory_space=pltpu.VMEM)
    operands = [where, coeffs, *whole, *operands]
    aliases = {}
    if result is not None:
        aliases = {len(operands): 0}
        operands.append(result)
    specs = [pl.BlockSpec(memory_space=pltpu.SMEM), vmem] + [hbm] * (len(operands) - 2)
    return pl.pallas_call(
        functools.partial(mix_kernel, len(whole), layout, tile, len(aliases)),
        out_shape=jax.ShapeDtypeStruct((size, cols), jnp.float32),
        in_specs=specs,
        out_specs=hbm,
        scratch_shapes=[pltpu.VMEM((size, extent), jnp.float32)] * (n + 1)
        + [pltpu.SemaphoreType.DMA((n, extent // tile)), pltpu.SemaphoreType.DMA((extent // tile,))],
        input_output_aliases=aliases,
        cost_estimate=pl.CostEstimate(
            flops=6 * 2 * n * size * size * extent, transcendentals=0,
            bytes_accessed=4 * (n + 1) * size * extent,
        ),
        name="mix",
    )(*operands)


def after(x, *deps):
    return lax.optimization_barrier((x, *deps))[0]


def widths(chips):
    return ((8, 4, 4), (8, 4, 4)) if chips == 2 else ((16,), (8, 8))


def early_of(chips):
    return 1 if chips == 2 else (chips - 1) ** 2


def starts_of(parts):
    return [sum(parts[:c]) for c in range(len(parts))]


def far_names(chips):
    others = range(1, chips)
    return [(o, p, c) for p in others for c in range(len(widths(chips)[1])) for o in others]


def on_device(snapshots, ref_index, weight_codes):
    own = snapshots[0]
    size, cols = own.shape
    n, mesh_size = lax.axis_size("variant"), lax.axis_size("mesh")
    chips = n // CORES
    part = cols // chips
    unit = part // 16
    me = lax.axis_index("variant").astype(jnp.int32)
    chip = me // CORES
    near_widths, far_widths = widths(chips)
    early = far_names(chips)[:early_of(chips)]
    scale = math.sqrt(cols * mesh_size)

    def move(x, offset):
        return lax.ppermute(x, "variant", xor_pairs(n, offset))

    def forward(x, *deps):
        return move(after(x, *deps), 1)

    def mesh_sum(x, beside=()):
        step, beside = 1, list(beside)
        while step < mesh_size:
            arrived = lax.ppermute(x, "mesh", xor_pairs(mesh_size, step))
            done = [beside.pop(0)(x)] if beside else []
            x = x + after(arrived, *done)
            step *= 2
        for call in beside:
            call(x)
        return x

    def gather(x):
        other = move(x, 1)
        both = jnp.concatenate([x, other], axis=0)
        blocks = [both]
        for offset in range(1, chips):
            blocks.append(move(both, CORES * offset))
        return blocks

    def piece_of(x, offset, start, width):
        return lax.dynamic_slice(
            x, (0, (chip ^ offset) * part + start * unit), (size, width * unit)
        )

    near, far = {}, {}
    where = me[None]
    near_starts, far_starts = starts_of(near_widths), starts_of(far_widths)
    for o in range(1, chips):
        near[o, 0] = move(piece_of(own, o, 0, near_widths[0]), CORES * o)
    partner = move(own, 1)
    own_gram = mmt(own, own)

    def send_near(c, source):
        for o in range(1, chips):
            piece = piece_of(source, o, near_starts[c], near_widths[c])
            near[o, c] = move(piece, CORES * o)
        return piece

    def send_far(o, p, c, source):
        piece = piece_of(source, o ^ p, far_starts[c], far_widths[c])
        far[o, p, c] = move(piece, CORES * o)
        return piece

    pair_gram = gram(
        where, lambda w: w[0] % CORES, [own, partner], [], [0], [(1,)], None, cols // CORES, 2048
    )
    calls = [lambda x, c=c: send_near(c, after(own, x)) for c in range(1, len(near_widths))]
    calls += [lambda x, key=key: send_far(*key, after(own, x)) for key in early]
    own_gram = mesh_sum(jnp.concatenate([own_gram, pair_gram], axis=1), calls)

    cross, others = None, {}
    ready = invert(own_gram) if len(near_widths) == 1 else own_gram
    for c, (start, width) in enumerate(zip(near_starts, near_widths)):
        dep = ready if cross is None else cross
        heads = [after(near[o, c], dep) for o in range(1, chips)]
        if c == 1:
            ready = invert(after(own_gram, cross))
            cross = after(cross, ready)
        columns, groups = [], [tuple(range(CORES))]
        for o in range(1, chips):
            near[o, c] = heads[o - 1]
        for o in range(1, chips - 1):
            others[o, c] = move(near[o, c], 1)
            columns.append(others[o, c])
        heads_at = [CORES + o for o in range(chips - 1)]
        for o in range(1, chips - 1):
            groups.append(groups[-1] + (heads_at[o - 1], CORES + chips - 1 + o - 1))
        cross = gram(
            where, lambda w, start=start, width=width: (w[0] // CORES * 16 + start) // width,
            [own, partner], heads + columns, heads_at, groups, cross, width * unit, 1024,
        )
    late = [key for key in far_names(chips) if key not in early]
    cross = mesh_sum(cross, [lambda x, key=key: send_far(*key, after(own, x)) for key in late])
    width = max(cross.shape[1], ready.shape[1])
    wide = lambda x: jnp.pad(x, ((0, 0), (0, width - x.shape[1])))
    gathered = gather(jnp.concatenate([wide(ready), wide(cross)], axis=0))
    coeffs = small(me[None], ref_index, weight_codes, gathered, size, scale)

    def at_near(start):
        return lambda w: w[0] // CORES * part + start * unit

    def at_far(p, start):
        return lambda w: (w[0] // CORES ^ p) * part + start * unit

    def far_parts(p, c, dep):
        parts = []
        for o in range(1, chips):
            parts += [far[o, p, c], forward(far[o, p, c], dep)]
        return at_far(p, far_starts[c]), parts

    chunks = []
    for c in range(len(near_widths)):
        parts = []
        for o in range(1, chips):
            other = others[o, c] if (o, c) in others else forward(near[o, c], cross)
            parts += [near[o, c], other]
        chunks.append((at_near(near_starts[c]), parts))
    places = [(p, c) for p in range(1, chips) for c in range(len(far_widths))]
    first = [(p, c) for p, c in places if all((o, p, c) in early for o in range(1, chips))]
    chunks += [far_parts(p, c, cross) for p, c in first]
    result = mix(where, coeffs, [own, partner], chunks, None, 2 * unit)
    results = [coeffs, result]
    for p, c in places:
        if (p, c) not in first:
            chunk = far_parts(p, c, results[-2])
            result = mix(where, coeffs, [own, partner], [chunk], result, 2 * unit)
            results.append(result)
    return result


def solution(mesh):
    return jax.shard_map(
        on_device,
        mesh=mesh,
        in_specs=(P("variant", None, "mesh"), P(), P()),
        out_specs=P(None, "mesh"),
        check_vma=False,
    )
```

```python
import functools
import math

import jax
import jax.numpy as jnp
from jax import lax
from jax.experimental import pallas as pl
from jax.experimental.pallas import tpu as pltpu
from jax.sharding import PartitionSpec as P


highest = lax.Precision.HIGHEST
atan_coeffs = [(-1.0) ** k / (2 * k + 1) for k in range(24)]
cos_coeffs = [(-1.0) ** k / math.factorial(2 * k) for k in range(24)]
sin_coeffs = [(-1.0) ** k / math.factorial(2 * k + 1) for k in range(24)]

CORES = 2
LOWEST = 1.0 / 1.64
STEP = 8
GRANT = 67043328


def xor_pairs(size, offset):
    return [(i, i ^ offset) for i in range(size)]


def mm(a, b):
    return jnp.dot(a, b, precision=highest, preferred_element_type=jnp.float32)


def mmt(a, b):
    return lax.dot_general(
        a, b, (((1,), (1,)), ((), ())), precision=highest, preferred_element_type=jnp.float32
    )


def powers_of(matrix, top):
    powers = {1: matrix}
    for k in range(2, top + 1):
        powers[k] = mm(powers[k // 2], powers[k - k // 2])
    return powers


def split(x):
    high = x.astype(jnp.bfloat16)
    rest = x - high.astype(jnp.float32)
    middle = rest.astype(jnp.bfloat16)
    low = (rest - middle.astype(jnp.float32)).astype(jnp.bfloat16)
    return high, middle, low


def raw_gram(a, b):
    return lax.dot_general(a, b, (((1,), (1,)), ((), ())), preferred_element_type=jnp.float32)


def raw_product(a, b):
    return jnp.dot(a, b, preferred_element_type=jnp.float32)


def fold(total, rows):
    tall = total.shape[0] // 3
    part = lambda i, j: total[i * tall:(i + 1) * tall, j * rows:(j + 1) * rows]
    order = sorted(((i, j) for i in range(3) for j in range(3)), key=lambda ij: -sum(ij))
    result = part(*order[0])
    for ij in order[1:]:
        result = result + part(*ij)
    return result


def load(refs, starts, slots, sems, tile):
    steps = slots[0].shape[1] // tile
    waits = []
    for t in range(steps):
        copies = []
        for index, (ref, start, slot) in enumerate(zip(refs, starts, slots)):
            first = start + t * tile
            if not isinstance(first, int):
                first = pl.multiple_of(first, 128)
            copies.append(
                pltpu.make_async_copy(
                    ref.at[:, pl.ds(first, tile)], slot.at[:, pl.ds(t * tile, tile)], sems.at[index, t]
                )
            )
            copies[-1].start()
        waits.append(copies)
    return waits


def gram_kernel(heads, groups, prior, at, whole, tile, where, *refs):
    count = (len(refs) - 2 - (1 if prior else 0)) // 2
    loaded, out = refs[:count], refs[count + (1 if prior else 0)]
    slots, sems = refs[-1 - count:-1], refs[-1]
    size, _ = slots[0].shape
    start = at(where)
    waits = load(loaded, [start] * whole + [0] * (count - whole), slots, sems, tile)
    totals = [None] * len(heads)
    for t, copies in enumerate(waits):
        for copy in copies:
            copy.wait()
        pieces = [split(slot[:, t * tile:(t + 1) * tile]) for slot in slots]
        for index, (head, columns) in enumerate(zip(heads, groups)):
            right = jnp.concatenate(pieces[head], axis=0)
            left = jnp.concatenate([pieces[g][level] for level in range(3) for g in columns], axis=0)
            value = raw_gram(left, right)
            totals[index] = value if totals[index] is None else totals[index] + value
    blocks = []
    for columns, total in zip(groups, totals):
        result = fold(total, size)
        blocks += [result[g * size:(g + 1) * size] for g in range(len(columns))]
    result = jnp.concatenate(blocks, axis=1)
    out[...] = result + refs[count][...] if prior else result


def gram(where, at, whole, parts, heads, groups, before, extent, tile, grant):
    size = (whole + parts)[0].shape[0]
    tile = min(tile, extent)
    width = sum(len(columns) for columns in groups) * size
    operands = [*whole, *parts]
    count = len(operands)
    vmem = pl.BlockSpec(memory_space=pltpu.VMEM)
    specs = [pl.BlockSpec(memory_space=pltpu.SMEM)] + [pl.BlockSpec(memory_space=pl.ANY)] * count
    if before is not None:
        operands.append(before)
        specs.append(vmem)
    return pl.pallas_call(
        functools.partial(gram_kernel, heads, groups, before is not None, at, len(whole), tile),
        out_shape=jax.ShapeDtypeStruct((size, width), jnp.float32),
        in_specs=specs,
        out_specs=vmem,
        scratch_shapes=[pltpu.VMEM((size, extent), jnp.float32)] * count
        + [pltpu.SemaphoreType.DMA((count, extent // tile))],
        cost_estimate=pl.CostEstimate(
            flops=9 * 2 * size * width * extent, transcendentals=0,
            bytes_accessed=4 * count * size * extent,
        ),
        compiler_params=pltpu.CompilerParams(vmem_limit_bytes=grant),
    )(where, *operands)


def invert_kernel(ref, out):
    size = ref.shape[0]
    rows = lax.broadcasted_iota(jnp.int32, (size, size), 0)
    cols = lax.broadcasted_iota(jnp.int32, (size, size), 1)
    eye = (rows == cols).astype(jnp.float32)
    index = lax.broadcasted_iota(jnp.int32, (size, 1), 0)
    work = jnp.concatenate([ref[:, :size], eye], axis=1)
    for j in range(size - 1):
        row = work[j:j + 1, :]
        factor = jnp.where(index > j, work[:, j:j + 1] / row[:, j:j + 1], 0.0)
        work = work - factor * row
    pivots = jnp.sum(work[:, :size] * eye, axis=1, keepdims=True)
    out[:, :size] = work[:, size:] / jnp.sqrt(pivots)
    out[:, size:] = ref[:, size:]


def invert(matrix):
    vmem = pl.BlockSpec(memory_space=pltpu.VMEM)
    return pl.pallas_call(
        invert_kernel,
        out_shape=jax.ShapeDtypeStruct(matrix.shape, jnp.float32),
        in_specs=[vmem],
        out_specs=vmem,
        cost_estimate=pl.CostEstimate(
            flops=4000 * matrix.shape[0] ** 2, bytes_accessed=8 * matrix.size, transcendentals=0
        ),
        name="invert",
    )(matrix)


def diagonal(packed, mask):
    return jnp.where(mask, jnp.concatenate([packed] * (mask.shape[0] // packed.shape[0]), axis=0), jnp.zeros((), packed.dtype))


def small_kernel(n, scale, me_ref, root_ref, code_ref, *refs):
    chips = n // CORES
    gathered, (out, gram_ref, corr) = refs[:chips], refs[chips:]
    size = out.shape[0]
    rows = gathered[0].shape[0] // CORES
    me = me_ref[0]
    root = root_ref[0] ^ me
    codes = [code_ref[j ^ me] for j in range(n)]
    eye = (
        lax.broadcasted_iota(jnp.int32, (size, size), 0)
        == lax.broadcasted_iota(jnp.int32, (size, size), 1)
    ).astype(jnp.float32)
    known = {}

    def add(row, col, block):
        if row > col:
            row, col, block = col, row, block.T
        known[row, col] = block if (row, col) not in known else known[row, col] + block

    lowers = []
    for s in range(n):
        chip, core = s // CORES, s % CORES
        ref, top = gathered[chip], core * rows
        lowers.append(ref[top:top + size, :size])
        add(s ^ 1, s, ref[top:top + size, size:CORES * size])
        column = 0
        for head in range(1, chips):
            for other in range(head):
                for g in range(CORES):
                    block = ref[top + size:top + 2 * size, column * size:(column + 1) * size]
                    add(CORES * (other ^ chip) + (core ^ g), CORES * (head ^ chip) + core, block)
                    column += 1
    zero = jnp.zeros((size, size), jnp.float32)
    for j in range(n):
        line = [zero if i == j else known[j, i] if j < i else known[i, j].T for i in range(n)]
        gram_ref[j * size:(j + 1) * size, :] = jnp.concatenate(line, axis=1)

    def block_mask(count):
        shape = (count * size, count * size)
        return (
            lax.broadcasted_iota(jnp.int32, shape, 0) // size
            == lax.broadcasted_iota(jnp.int32, shape, 1) // size
        )

    group = CORES
    wide = group * size
    every, mask = block_mask(n), block_mask(group)
    lower = jnp.concatenate(lowers, axis=1)
    spread = diagonal(lower, every)
    shape = (n * size, n * size)
    whole_eye = (
        lax.broadcasted_iota(jnp.int32, shape, 0) == lax.broadcasted_iota(jnp.int32, shape, 1)
    ).astype(jnp.float32)
    corr[...] = jnp.where(every, whole_eye, mmt(mm(spread, gram_ref[...]), spread))
    to_root = corr[pl.ds(pl.multiple_of(root * size, size), size), :]

    middle = 2.0 / (1.0 + LOWEST)
    eyes = jnp.concatenate([eye] * group, axis=1)
    lane = lax.broadcasted_iota(jnp.int32, (1, wide), 1) // size

    def each(a, b, product=raw_product):
        high, middle, low = [diagonal(x, mask) for x in split(b)]
        left = jnp.concatenate(split(a), axis=0)
        one = product(left, jnp.concatenate([high, middle], axis=product is raw_product))
        two = product(left[:size], low)
        little = one[2 * size:, :wide] + one[size:2 * size, wide:] + two
        return (little + (one[size:2 * size, :wide] + one[:size, wide:])) + one[:size, :wide]

    def groups(x):
        return [x[:, first * size:first * size + wide] for first in range(0, n, group)]

    terms, phi = [], zero
    for number, m in enumerate(groups(to_root)):
        k = each(m, m, raw_gram)
        r = eyes - middle * k
        r2 = each(r, r)
        total = each(eyes + r, eyes + r2)
        r4 = each(r2, r2)
        total = each(total, eyes + r4)
        r8 = each(r4, r4)
        inv = middle * each(total, eyes + r8)
        right = each(inv, m)
        powers = {1: inv - eyes}
        for p in range(2, STEP + 1):
            powers[p] = each(powers[p // 2], powers[p - p // 2])
        factor = None
        for start in reversed(range(0, len(atan_coeffs), STEP)):
            block = atan_coeffs[start] * eyes
            for p in range(1, min(STEP, len(atan_coeffs) - start)):
                block = block + atan_coeffs[start + p] * powers[p]
            factor = block if factor is None else block + each(powers[STEP], factor)
        weight = jnp.zeros((1, wide), jnp.int32)
        for g in range(group):
            weight = jnp.where(lane == g, codes[number * group + g], weight)
        all_codes = jnp.full((1, wide), sum(codes), jnp.int32)
        factor = (weight.astype(jnp.float32) / all_codes.astype(jnp.float32)) * factor
        for g in range(group):
            phi = phi + factor[:, g * size:(g + 1) * size]
        terms.append(each(factor, right))
    term = jnp.concatenate(terms, axis=1)
    energy = mmt(mm(term, corr[...]), term) - mm(phi, phi)
    at_root = lax.broadcasted_iota(jnp.int32, (1, n * size), 1) // size == root
    term = term - jnp.where(at_root, jnp.concatenate([phi] * n, axis=1), 0.0)
    right = [each(a, b) for a, b in zip(groups(term), groups(lower))]
    stacked = jnp.concatenate(
        [jnp.where(at_root, lower, 0.0), jnp.concatenate(right, axis=1)], axis=0
    )
    powers = powers_of(energy, STEP)
    both = [
        jnp.concatenate([jnp.full((1, size), c), jnp.full((1, size), s)], axis=1)
        for c, s in zip(cos_coeffs, sin_coeffs)
    ]
    twice = {p: jnp.concatenate([power] * 2, axis=1) for p, power in powers.items()}
    total = None
    for start in reversed(range(0, len(both), STEP)):
        block = both[start] * jnp.concatenate([eye] * 2, axis=1)
        for p in range(1, min(STEP, len(both) - start)):
            block = block + both[start + p] * twice[p]
        total = block if total is None else block + mm(powers[STEP], total)
    out[...] = scale * mm(total, stacked)


def small(me, root, codes, gathered, size, scale):
    n = len(gathered) * CORES
    vmem = pl.BlockSpec(memory_space=pltpu.VMEM)
    smem = pl.BlockSpec(memory_space=pltpu.SMEM)
    return pl.pallas_call(
        functools.partial(small_kernel, n, scale),
        out_shape=jax.ShapeDtypeStruct((size, n * size), jnp.float32),
        in_specs=[smem, smem, smem] + [vmem] * len(gathered),
        out_specs=vmem,
        scratch_shapes=[pltpu.VMEM((n * size, n * size), jnp.float32)] * 2,
        cost_estimate=pl.CostEstimate(
            flops=20000 * size**3, bytes_accessed=4 * 4 * n * size * size, transcendentals=0
        ),
        name="small",
    )(me, root, codes, *gathered)


def mix_kernel(whole, chunks, tile, aliased, where, coeffs, *refs):
    loaded = refs[:whole + sum(count for _, count, _ in chunks)]
    slots = refs[-3 - whole - chunks[0][1]:-3]
    out, (sums, in_sems, out_sems) = refs[len(loaded) + aliased], refs[-3:]
    size = sums.shape[0]
    waits, places, begun = [], [], whole
    for at, count, width in chunks:
        group = loaded[:whole] + loaded[begun:begun + count]
        begun += count
        for t in range(width // tile):
            number, copies = len(waits), []
            place = pl.ds(pl.multiple_of(at(where) + t * tile, 128), tile)
            for index, (ref, slot) in enumerate(zip(group, slots)):
                copies.append(
                    pltpu.make_async_copy(
                        ref.at[:, place if index < whole else pl.ds(t * tile, tile)],
                        slot.at[:, pl.ds(number * tile, tile)],
                        in_sems.at[index, number],
                    )
                )
                copies[-1].start()
            waits.append(copies)
            places.append(place)
    left = jnp.concatenate(split(coeffs[...]), axis=0)
    stores = []
    for t, copies in enumerate(waits):
        for copy in copies:
            copy.wait()
        here = slice(t * tile, (t + 1) * tile)
        high, middle, low = split(jnp.concatenate([slot[:, here] for slot in slots], axis=0))
        one = jnp.dot(left, high, preferred_element_type=jnp.float32)
        two = jnp.dot(left[:2 * size], middle, preferred_element_type=jnp.float32)
        three = jnp.dot(left[:size], low, preferred_element_type=jnp.float32)
        little = one[2 * size:] + two[size:] + three
        sums[:, here] = (little + (one[size:2 * size] + two[:size])) + one[:size]
        stores.append(
            pltpu.make_async_copy(
                sums.at[:, pl.ds(t * tile, tile)],
                out.at[:, places[t]],
                out_sems.at[t],
            )
        )
        stores[-1].start()
    for store in stores:
        store.wait()


def mix(where, coeffs, whole, chunks, result, tile):
    size, cols = whole[0].shape
    n = len(whole) + len(chunks[0][1])
    layout, extent, operands = [], 0, []
    for at, parts in chunks:
        layout.append((at, len(parts), parts[0].shape[1]))
        extent += parts[0].shape[1]
        operands += parts
    hbm = pl.BlockSpec(memory_space=pl.ANY)
    vmem = pl.BlockSpec(memory_space=pltpu.VMEM)
    operands = [where, coeffs, *whole, *operands]
    aliases = {}
    if result is not None:
        aliases = {len(operands): 0}
        operands.append(result)
    specs = [pl.BlockSpec(memory_space=pltpu.SMEM), vmem] + [hbm] * (len(operands) - 2)
    return pl.pallas_call(
        functools.partial(mix_kernel, len(whole), layout, tile, len(aliases)),
        out_shape=jax.ShapeDtypeStruct((size, cols), jnp.float32),
        in_specs=specs,
        out_specs=hbm,
        scratch_shapes=[pltpu.VMEM((size, extent), jnp.float32)] * (n + 1)
        + [pltpu.SemaphoreType.DMA((n, extent // tile)), pltpu.SemaphoreType.DMA((extent // tile,))],
        input_output_aliases=aliases,
        cost_estimate=pl.CostEstimate(
            flops=6 * 2 * n * size * size * extent, transcendentals=0,
            bytes_accessed=4 * (n + 1) * size * extent,
        ),
        compiler_params=pltpu.CompilerParams(vmem_limit_bytes=GRANT),
        name="mix",
    )(*operands)


def after(x, *deps):
    return lax.optimization_barrier((x, *deps))[0]


def widths(chips):
    return ((8, 6, 2), (8, 6, 2)) if chips == 2 else ((16,), (8, 8))


def early_of(chips):
    return 1 if chips == 2 else (chips - 1) ** 2


def starts_of(parts):
    return [sum(parts[:c]) for c in range(len(parts))]


def far_names(chips):
    others = range(1, chips)
    return [(o, p, c) for p in others for c in range(len(widths(chips)[1])) for o in others]


def on_device(snapshots, ref_index, weight_codes):
    own = snapshots[0]
    size, cols = own.shape
    n, mesh_size = lax.axis_size("variant"), lax.axis_size("mesh")
    chips = n // CORES
    part = cols // chips
    unit = part // 16
    me = lax.axis_index("variant").astype(jnp.int32)
    chip = me // CORES
    near_widths, far_widths = widths(chips)
    early = far_names(chips)[:early_of(chips)]
    scale = math.sqrt(cols * mesh_size)

    def move(x, offset):
        return lax.ppermute(x, "variant", xor_pairs(n, offset))

    def forward(x, *deps):
        return move(after(x, *deps), 1)

    def mesh_sum(x, beside=()):
        step, beside = 1, list(beside)
        while step < mesh_size:
            arrived = lax.ppermute(x, "mesh", xor_pairs(mesh_size, step))
            done = [beside.pop(0)(x)] if beside else []
            x = x + after(arrived, *done)
            step *= 2
        for call in beside:
            call(x)
        return x

    def gather(x):
        other = move(x, 1)
        both = jnp.concatenate([x, other], axis=0)
        blocks = [both]
        for offset in range(1, chips):
            blocks.append(move(both, CORES * offset))
        return blocks

    def piece_of(x, offset, start, width):
        return lax.dynamic_slice(
            x, (0, (chip ^ offset) * part + start * unit), (size, width * unit)
        )

    near, far = {}, {}
    where = me[None]
    near_starts, far_starts = starts_of(near_widths), starts_of(far_widths)
    for o in range(1, chips):
        near[o, 0] = move(piece_of(own, o, 0, near_widths[0]), CORES * o)
    partner = move(own, 1)
    own_gram = mmt(own, own)

    def send_near(c, source):
        for o in range(1, chips):
            piece = piece_of(source, o, near_starts[c], near_widths[c])
            near[o, c] = move(piece, CORES * o)
        return piece

    def send_far(o, p, c, source):
        piece = piece_of(source, o ^ p, far_starts[c], far_widths[c])
        far[o, p, c] = move(piece, CORES * o)
        return piece

    pair_gram = gram(
        where, lambda w: w[0] % CORES * (cols // CORES), [own, partner], [], [0], [(1,)], None, cols // CORES, 2048, GRANT
    )
    calls = [lambda x, c=c: send_near(c, after(own, x)) for c in range(1, len(near_widths))]
    calls += [lambda x, key=key: send_far(*key, after(own, x)) for key in early]
    own_gram = mesh_sum(jnp.concatenate([own_gram, pair_gram], axis=1), calls)

    cross, others, crosses = None, {}, []
    ready = invert(own_gram) if len(near_widths) == 1 else own_gram
    for c, (start, width) in enumerate(zip(near_starts, near_widths)):
        dep = ready if cross is None else cross
        heads = [after(near[o, c], dep) for o in range(1, chips)]
        if c == 1:
            ready = invert(after(own_gram, cross))
            cross = after(cross, ready)
        columns, groups = [], [tuple(range(CORES))]
        for o in range(1, chips):
            near[o, c] = heads[o - 1]
        for o in range(1, chips - 1):
            others[o, c] = move(near[o, c], 1)
            columns.append(others[o, c])
        heads_at = [CORES + o for o in range(chips - 1)]
        for o in range(1, chips - 1):
            groups.append(groups[-1] + (heads_at[o - 1], CORES + chips - 1 + o - 1))
        cross = gram(
            where, lambda w, start=start: w[0] // CORES * part + start * unit,
            [own, partner], heads + columns, heads_at, groups, cross, width * unit, 1024,
            GRANT if c < len(near_widths) - 1 else None,
        )
        crosses.append(cross)
    late = [key for key in far_names(chips) if key not in early]
    cross = mesh_sum(cross, [lambda x, key=key: send_far(*key, after(own, x)) for key in late])
    width = max(cross.shape[1], ready.shape[1])
    wide = lambda x: jnp.pad(x, ((0, 0), (0, width - x.shape[1])))
    gathered = gather(jnp.concatenate([wide(ready), wide(cross)], axis=0))
    coeffs = small(me[None], ref_index, weight_codes, gathered, size, scale)

    def at_near(start):
        return lambda w: w[0] // CORES * part + start * unit

    def at_far(p, start):
        return lambda w: (w[0] // CORES ^ p) * part + start * unit

    def far_parts(p, c, dep):
        parts = []
        for o in range(1, chips):
            parts += [far[o, p, c], forward(far[o, p, c], dep)]
        return at_far(p, far_starts[c]), parts

    chunks = []
    for c in range(len(near_widths)):
        parts = []
        for o in range(1, chips):
            other = others[o, c] if (o, c) in others else forward(near[o, c], crosses[c])
            parts += [near[o, c], other]
        chunks.append((at_near(near_starts[c]), parts))
    places = [(p, c) for p in range(1, chips) for c in range(len(far_widths))]
    first = [(p, c) for p, c in places if all((o, p, c) in early for o in range(1, chips))]
    result = mix(where, coeffs, [own, partner], chunks, None, 2 * unit)
    results = [coeffs, result]
    for p, c in places:
        chunk = far_parts(p, c, cross if (p, c) in first else results[-2])
        result = mix(where, coeffs, [own, partner], [chunk], result, 2 * unit)
        results.append(result)
    return result


def solution(mesh):
    return jax.shard_map(
        on_device,
        mesh=mesh,
        in_specs=(P("variant", None, "mesh"), P(), P()),
        out_specs=P(None, "mesh"),
        check_vma=False,
    )
```
